512 devices in a mesh: lat: 64 (over y, z), ma: 8 (over x, core).
Axes of the slice: x: 4, y: 8, z: 8, core: 2. Of those that a mesh axis runs over, the one named last changes fastest.
Arguments:
- pair_wave: int32 [360], replicated, may hold values from 0 to 359, each once
- legendre: bfloat16 [360, 640, 768], P('ma', 'lat'), may hold values from -0.0078125 to 0.0078125
- coefs: bfloat16 [360, 768, 168], P('ma', 'lat'), may hold values from -6 to 6
Outputs:
- noise: float32 [53760, 1440], P(('lat', 'ma'))
The draws below stay inside these ranges and needn't reach their ends.
Inputs may be any that keep to these rules, and one draw needn't show every extreme that they name: Slot q holds wavenumbers pair_wave[q] and 719 - pair_wave[q]; every value appears once.
All inputs are finite; a program needn't handle non-finite values.
Results may differ from the reference program's by a relative error of at most 0.0003.
Values may be sent and summed in bfloat16 or wider, within the bound.
A program may use at most 64 MiB of HBM per device.

```python
import math
import jax
import jax.numpy as jnp
from jax import lax

DEG = 720
LON = 1440
CH = 84
LAT_DEV = 10
PAIRS = 360
RROWS = 768
COLS = 168
LATS = 640
N_LAT = 64
N_MA = 8


def level_of(key, dims, split, smallest, high):
    factor_of = 1.0
    for axis_at, shards_of in split:
        draws = jax.random.uniform(jax.random.fold_in(jax.random.fold_in(key, 6), axis_at), (shards_of,), jnp.float32, smallest / len(split), high / len(split))
        factor_of = factor_of * jnp.repeat(jnp.exp(draws), dims[axis_at] // shards_of).reshape((-1,) + (1,) * (len(dims) - 1 - axis_at))
    return factor_of


def noise(stream_key, extent, deviation, most, shards=(), kind=jnp.bfloat16):
    values = jax.random.normal(stream_key, extent, jnp.float32) * deviation
    if len(shards) > 0:
        values = level_of(stream_key, extent, shards, -0.22, 0.18) * values
    return jnp.clip(values, min=-most, max=most).astype(kind)


def setup_inputs(seed: int = 0) -> dict:
    key_list = jax.random.split(jax.random.key(seed), 4)
    pair_wave = jax.random.permutation(key_list[0], PAIRS).astype(jnp.int32)
    legendre = noise(key_list[1], (PAIRS, LATS, RROWS), (RROWS * DEG) ** -0.5, 0.0078125, ((0, 8), (1, 64)))
    coefs = noise(key_list[2], (PAIRS, RROWS, COLS), 1.0, 6.0, ((0, 8), (1, 64)))
    return dict(pair_wave=pair_wave, legendre=legendre, coefs=coefs)


def chain_table(table, wave_ids, degree_top):
    row_count = table.shape[2]
    row_ids = jnp.arange(row_count, dtype=jnp.int32)[None, :]
    split_row = (degree_top - wave_ids).astype(jnp.int32)[:, None]
    inside = row_ids < split_row
    outside = (row_ids >= split_row) & (row_ids <= degree_top)
    masks = jnp.stack([inside, outside], axis=1)
    return jnp.where(masks[:, :, None, :], table[:, None, :, :], jnp.zeros((), table.dtype))


def fourier_basis(pair_wave, degree_top, lon_count):
    orders = jnp.stack([pair_wave, degree_top - 1 - pair_wave], axis=1).astype(jnp.int32)
    positions = jnp.arange(lon_count, dtype=jnp.int32)
    phase_int = (orders[:, :, None] * positions[None, None, :]) % lon_count
    radians = (2.0 * math.pi / lon_count) * phase_int.astype(jnp.float32)
    weight = jnp.where(orders == 0, 1.0, 2.0).astype(jnp.float32)[:, :, None]
    real_row = weight * jnp.cos(radians)
    imag_row = -weight * jnp.sin(radians)
    return jnp.stack([real_row, imag_row], axis=2).reshape(-1, lon_count)


def reference(pair_wave, legendre, coefs):
    pair_count = pair_wave.shape[0]
    row_count = coefs.shape[1]
    lat_total = LAT_DEV * N_LAT
    slot_count = pair_count // N_MA

    def group_spectra(packed):
        wave_ids, group_table, group_coefs = packed
        masked = chain_table(group_table, wave_ids, DEG)
        return jnp.einsum('qeir,qrc->qeic', masked.astype(jnp.float32), group_coefs.astype(jnp.float32), precision=lax.Precision.HIGHEST)

    spectra = lax.map(group_spectra, (pair_wave.reshape(N_MA, slot_count), legendre.reshape(N_MA, slot_count, lat_total, row_count), coefs.reshape(N_MA, slot_count, row_count, coefs.shape[2])))
    spectra = spectra.reshape(pair_count, 2, lat_total, 2, CH)
    fourier_rows = jnp.transpose(spectra, (0, 1, 3, 2, 4)).reshape(4 * pair_count, lat_total * CH)
    synth_basis = fourier_basis(pair_wave, DEG, LON)
    return lax.dot_general(fourier_rows, synth_basis, (((0,), (0,)), ((), ())), precision=lax.Precision.HIGHEST)
```

```python
import math

import jax
import jax.numpy as jnp
from jax import lax
from jax.experimental import pallas as pl
from jax.experimental.pallas import tpu as pltpu
from jax.sharding import PartitionSpec as P

DEG = 720
LON = 1440
HALF = LON // 2
CH = 84
LAT_DEV = 10
CHUNK = LAT_DEV * CH // 8
MESH = pl.DeviceIdType.MESH
ORDER = (4, 3, 5, 2, 6, 1, 7)
ROWS = 1024
BLK = 64


def wave_rows(pw_ref, tab_ref):
    pw = pw_ref[...]
    half = jnp.broadcast_to((pw >> 1).astype(jnp.float32).astype(jnp.bfloat16), (128, 384))
    low = jnp.broadcast_to((pw & 1).astype(jnp.float32).astype(jnp.bfloat16), (128, 384))

    def step(b, _):
        row = lax.broadcasted_iota(jnp.int32, (256, 384), 0) + b * 256
        col = lax.broadcasted_iota(jnp.int32, (256, 384), 1)
        group = row >> 3
        slot = 3 * (group & 15) + ((row & 7) >> 1)
        slot = (group >> 4) * 45 + jnp.where((slot < 45) & ((row & 7) < 6), slot, 0)
        pick = jnp.where(col == slot, 1.0, 0.0).astype(jnp.bfloat16)
        dims = (((1,), (1,)), ((), ()))
        hi = lax.dot_general(pick, half, dims, preferred_element_type=jnp.float32)
        lo = lax.dot_general(pick, low, dims, preferred_element_type=jnp.float32)
        tab_ref[pl.ds(pl.multiple_of(b * 256, 256), 256), :] = 2.0 * hi + lo
        return 0

    lax.fori_loop(0, ROWS // 256, step, 0)


def cos_sin(phase):
    turns = jnp.floor(phase * (1.0 / LON))
    t = (phase - turns * LON - HALF) * (2.0 * math.pi / LON / 4.0)
    q = t * t
    s = t * (1.0 + q * (-1.0 / 6 + q * (1.0 / 120 + q * (-1.0 / 5040 + q * (1.0 / 362880)))))
    c = 1.0 + q * (-0.5 + q * (1.0 / 24 + q * (-1.0 / 720 + q * (1.0 / 40320 - q * (1.0 / 3628800)))))
    s, c = 2.0 * s * c, 1.0 - 2.0 * s * s
    s, c = 2.0 * s * c, 1.0 - 2.0 * s * s
    return -c, -s


def basis_block(b, tab_ref, hi_ref, lo_ref):
    start = pl.multiple_of(b * BLK, BLK)
    u = tab_ref[pl.ds(start, BLK), :]
    lane = lax.broadcasted_iota(jnp.int32, (BLK, 128), 1).astype(jnp.float32)
    part = (lax.broadcasted_iota(jnp.int32, (BLK, 128), 0) & 1).astype(jnp.float32)
    odd = u - 2.0 * jnp.floor(u * 0.5)
    for h in range(2):
        wave = jnp.where(odd == float(h), u, float(DEG - 1) - u)
        c, s = cos_sin(wave * lane + 360.0 * part)
        weight = jnp.where(wave == 0.0, 1.0, 2.0)
        c, s = c * weight, s * weight
        cj, sj = cos_sin(wave * 128.0)
        for j in range(6):
            high = c.astype(jnp.bfloat16)
            hi_ref[h, pl.ds(start, BLK), 128 * j : 128 * j + 128] = high
            lo_ref[h, pl.ds(start, BLK), 128 * j : 128 * j + 128] = (c - high.astype(jnp.float32)).astype(jnp.bfloat16)
            if j < 5:
                c, s = c * cj - s * sj, s * cj + c * sj


def legendre_sums(waves, table_ref, coef_ref, sums_ref, out_ref):
    table = table_ref[...].reshape(256, 768)
    row = lax.broadcasted_iota(jnp.int32, (768, 168), 0)
    for s in range(3):
        coefs = coef_ref[..., 168 * s : 168 * s + 168].reshape(768, 168)
        u = waves[s]
        odd = lax.rem(u, 2)
        first = DEG - u
        for h in range(2):
            low = jnp.where(odd == h, 0, first)
            high = jnp.where(odd == h, first, DEG + 1)
            kept = jnp.where((row >= low) & (row < high), coefs, jnp.zeros((), coefs.dtype))
            sums = jnp.dot(table, kept, preferred_element_type=jnp.float32)
            for e in range(2):
                sums_ref[6 * h + 2 * s + e, :, 0:CH] = sums[:, CH * e : CH * e + CH]
    lane = lax.broadcasted_iota(jnp.int32, (8, 128), 1)
    for h in range(2):
        for s in range(3):
            for e in range(2):
                lats = [
                    sums_ref[6 * h + 2 * s + e, pl.ds(LAT_DEV * s + i, 8, stride=32), :] for i in range(LAT_DEV)
                ]
                for k in range(8):
                    i, off = divmod(CHUNK * k, CH)
                    a = lats[i] if off == 0 else pltpu.roll(lats[i], 128 - off, 1)
                    b = pltpu.roll(lats[i + 1], CH - off, 1)
                    chunk = jnp.where(lane < CH - off, a, b)
                    out_ref[pl.ds(16 * k + 8 * h + 2 * s + e, 8, stride=128), :] = chunk


def kernel(pw_s, pw_v, table_in, coef_in, out_ref, tab, hi, lo, table_a, table_b, coef_a, coef_b, sums_s, send, home, held,
           cs, cr, ts, tr, rs, rr, fs, fr, ms, mr):
    lat = lax.axis_index("lat")
    ma = lax.axis_index("ma")
    y, z = lat // 8, lax.rem(lat, 8)
    along_z = [(y * 8 + lax.rem(z + d, 8), ma) for d in range(8)]
    along_y = [(lax.rem(y + d, 8) * 8 + z, ma) for d in range(8)]
    along_ma = [(lat, lax.rem(ma + d, 8)) for d in range(8)]

    barrier = pltpu.get_barrier_semaphore()
    for peers in (along_z, along_y, along_ma):
        for d in range(1, 8):
            pl.semaphore_signal(barrier, inc=1, device_id=peers[d], device_id_type=MESH)
    wave_rows(pw_v, tab)
    send[...] = jnp.zeros_like(send)
    pl.semaphore_wait(barrier, 21)

    def copy(src, dst, s_sem, r_sem, to):
        return pltpu.make_async_remote_copy(
            src_ref=src, dst_ref=dst, send_sem=s_sem, recv_sem=r_sem, device_id=to, device_id_type=MESH
        )

    waits = []
    first = []
    for d in ORDER:
        za, yb = lax.rem(z + d, 8), lax.rem(y + d, 8)
        a = copy(coef_in.at[za], coef_a.at[y, z], cs.at[0, d], cr.at[0, d], along_z[d])
        b = copy(coef_in.at[8 + yb], coef_b.at[y, z], cs.at[1, d], cr.at[1, d], along_y[d])
        a.start()
        b.start()
        first += [a, b]
    coef_a[y, z] = coef_in[z]
    coef_b[y, z] = coef_in[8 + y]

    tables = []

    def send_tables(ds):
        for d in ds:
            za, yb = lax.rem(z + d, 8), lax.rem(y + d, 8)
            a = copy(table_in.at[za], table_a.at[z], ts.at[0, d], tr.at[0, d], along_z[d])
            b = copy(table_in.at[8 + yb], table_b.at[y], ts.at[1, d], tr.at[1, d], along_y[d])
            a.start()
            b.start()
            tables.extend([a, b])

    def basis(lo_b, hi_b):
        def step(b, _):
            basis_block(b, tab, hi, lo)
            return 0

        lax.fori_loop(lo_b, hi_b, step, 0)

    send_tables(ORDER[:2])
    basis(0, 3)
    for c in first:
        c.wait_recv()
    waits += first

    for s in range(4):
        now = []
        for way in range(2):
            if way == 1 and s == 3:
                continue
            sign = 1 if way == 0 else 7
            by, bz = lax.rem(y + (8 - sign) * s, 8), lax.rem(z + (8 - sign) * s, 8)
            a = copy(coef_a.at[by], coef_a.at[by], rs.at[0, way, s], rr.at[0, way, s], along_y[sign])
            b = copy(coef_b.at[:, bz], coef_b.at[:, bz], rs.at[1, way, s], rr.at[1, way, s], along_z[sign])
            a.start()
            b.start()
            now += [a, b]
        send_tables(ORDER[2 + 2 * s : 4 + 2 * s] if s < 2 else ORDER[6:7] if s == 2 else ())
        basis(3 + 3 * s, 6 + 3 * s if s < 3 else ROWS // BLK)
        for c in now:
            c.wait_recv()
        waits += now
    table_a[z] = table_in[z]
    table_b[y] = table_in[8 + y]

    sums = []
    for half, (table, coef, mine, peers) in enumerate(
        ((table_a, coef_a, z, along_z), (table_b, coef_b, y, along_y))
    ):
        for c in tables[half::2]:
            c.wait_recv()
        at = ma * 45 + half * 24 + mine * 3
        waves = [pw_s[jnp.minimum(at + s, 359)] for s in range(3)]
        legendre_sums(waves, table, coef, sums_s, send.at[half])
        for d in ORDER:
            to = lax.rem(mine + d, 8)
            c = copy(
                send.at[half, pl.ds(pl.multiple_of(to * 128, 128), 128)],
                home.at[half * 8 + mine],
                fs.at[half, d],
                fr.at[half, d],
                peers[d],
            )
            c.start()
            sums.append(c)
        home[half * 8 + mine] = send[half, pl.ds(pl.multiple_of(mine * 128, 128), 128)]
    waits += tables
    for c in sums:
        c.wait_recv()
    waits += sums

    final = []
    for d in ORDER:
        to = lax.rem(ma + d, 8)
        c = copy(
            home.at[:, pl.ds(pl.multiple_of(to * 16, 16), 16)], held.at[ma], ms.at[d], mr.at[d], along_ma[d]
        )
        c.start()
        final.append(c)
    held[ma] = home[:, pl.ds(pl.multiple_of(ma * 16, 16), 16), :]
    for c in final:
        c.wait_recv()
    waits += final
    for c in waits:
        c.wait_send()

    dims = (((0,), (0,)), ((), ()))
    halves = []
    for h in range(2):
        x = held[:, :, 8 * h : 8 * h + 8, :].reshape(ROWS, 128)
        high = x.astype(jnp.bfloat16)
        low = (x - high.astype(jnp.float32)).astype(jnp.bfloat16)
        total = lax.dot_general(high, hi[h], dims, preferred_element_type=jnp.float32)
        total += lax.dot_general(low, hi[h], dims, preferred_element_type=jnp.float32)
        total += lax.dot_general(high, lo[h], dims, preferred_element_type=jnp.float32)
        halves.append(total)
    out_ref[:, 0:HALF] = (halves[0] + halves[1])[:CHUNK, :HALF]
    out_ref[:, HALF:LON] = (halves[0] - halves[1])[:CHUNK, :HALF]


def body(pair_wave, legendre, coefs):
    table = jnp.pad(legendre, ((0, 3), (0, 0), (0, 0))).reshape(16, 30, 768)
    table = jnp.pad(table, ((0, 0), (0, 2), (0, 0)))
    coef = jnp.pad(coefs, ((0, 3), (0, 0), (0, 0))).reshape(16, 3, 12, 168)
    coef = jnp.transpose(coef, (0, 2, 1, 3)).reshape(16, 12, 504)
    coef = jnp.pad(coef, ((0, 0), (0, 0), (0, 8))).reshape(16, 3, 4, 512)
    pw_v = jnp.pad(pair_wave, (0, 24)).reshape(1, 384)
    vmem = pl.BlockSpec(memory_space=pltpu.VMEM)
    bf16, f32, dma = jnp.bfloat16, jnp.float32, pltpu.SemaphoreType.DMA
    return pl.pallas_call(
        kernel,
        out_shape=jax.ShapeDtypeStruct((CHUNK, LON), f32),
        in_specs=[pl.BlockSpec(memory_space=pltpu.SMEM), vmem, vmem, vmem],
        out_specs=vmem,
        scratch_shapes=[
            pltpu.VMEM((ROWS, 128), f32),
            pltpu.VMEM((2, ROWS, 768), bf16),
            pltpu.VMEM((2, ROWS, 768), bf16),
            pltpu.VMEM((8, 32, 768), bf16),
            pltpu.VMEM((8, 32, 768), bf16),
            pltpu.VMEM((8, 8, 3, 4, 512), bf16),
            pltpu.VMEM((8, 8, 3, 4, 512), bf16),
            pltpu.VMEM((12, 256, 128), f32),
            pltpu.VMEM((2, 1024, 128), f32),
            pltpu.VMEM((16, 128, 128), f32),
            pltpu.VMEM((8, 16, 16, 128), f32),
            dma((2, 8)), dma((2, 8)), dma((2, 8)), dma((2, 8)),
            dma((2, 2, 4)), dma((2, 2, 4)), dma((2, 8)), dma((2, 8)), dma((8,)), dma((8,)),
        ],
        compiler_params=pltpu.CompilerParams(
            collective_id=0, has_side_effects=True, vmem_limit_bytes=60 * 2**20
        ),
    )(pair_wave, pw_v, table, coef)


def solution(mesh):
    placed = (P(), P("ma", "lat", None), P("ma", "lat", None))
    return jax.shard_map(
        body, mesh=mesh, in_specs=placed, out_specs=P(("lat", "ma"), None), check_vma=False
    )
```

```python
import math

import jax
import jax.numpy as jnp
from jax import lax
from jax.experimental import pallas as pl
from jax.experimental.pallas import tpu as pltpu
from jax.sharding import PartitionSpec as P

DEG = 720
LON = 1440
HALF = LON // 2
CH = 84
LAT_DEV = 10
CHUNK = LAT_DEV * CH // 8
MESH = pl.DeviceIdType.MESH
ORDER = (4, 3, 5, 2, 6, 1, 7)
ROWS = 1024
BLK = 64


def wave_rows(pw_s, pw_v, tab_ref):
    lane = lax.broadcasted_iota(jnp.int32, (8, 128), 1)
    for t in range(3):

        def gather(n, v):
            for k in range(8):
                at = t * 128 + n * 8 + k
                v = jnp.where(lane == n * 8 + k, pw_s[jnp.minimum(at, 359)], v)
            return v

        pw_v[:, 128 * t : 128 * t + 128] = lax.fori_loop(0, 16, gather, jnp.zeros((8, 128), jnp.int32))
    pw = pw_v[0:1, :]
    half = jnp.broadcast_to((pw >> 1).astype(jnp.float32).astype(jnp.bfloat16), (128, 384))
    low = jnp.broadcast_to((pw & 1).astype(jnp.float32).astype(jnp.bfloat16), (128, 384))

    def step(b, _):
        row = lax.broadcasted_iota(jnp.int32, (256, 384), 0) + b * 256
        col = lax.broadcasted_iota(jnp.int32, (256, 384), 1)
        group = row >> 3
        slot = 24 * (group >> 6) + 3 * (group & 7) + ((row & 7) >> 1)
        slot = ((group >> 3) & 7) * 45 + jnp.where((slot < 45) & ((row & 7) < 6), slot, 0)
        pick = jnp.where(col == slot, 1.0, 0.0).astype(jnp.bfloat16)
        dims = (((1,), (1,)), ((), ()))
        hi = lax.dot_general(pick, half, dims, preferred_element_type=jnp.float32)
        lo = lax.dot_general(pick, low, dims, preferred_element_type=jnp.float32)
        tab_ref[pl.ds(pl.multiple_of(b * 256, 256), 256), :] = 2.0 * hi + lo
        return 0

    lax.fori_loop(0, ROWS // 256, step, 0)


def cos_sin(phase):
    turns = jnp.floor(phase * (1.0 / LON))
    t = (phase - turns * LON - HALF) * (2.0 * math.pi / LON / 4.0)
    q = t * t
    s = t * (1.0 + q * (-1.0 / 6 + q * (1.0 / 120 + q * (-1.0 / 5040 + q * (1.0 / 362880)))))
    c = 1.0 + q * (-0.5 + q * (1.0 / 24 + q * (-1.0 / 720 + q * (1.0 / 40320 - q * (1.0 / 3628800)))))
    s, c = 2.0 * s * c, 1.0 - 2.0 * s * s
    s, c = 2.0 * s * c, 1.0 - 2.0 * s * s
    return -c, -s


def basis_block(b, tab_ref, hi_ref, lo_ref):
    start = pl.multiple_of(b * BLK, BLK)
    u = tab_ref[pl.ds(start, BLK), :]
    lane = lax.broadcasted_iota(jnp.int32, (BLK, 128), 1).astype(jnp.float32)
    part = (lax.broadcasted_iota(jnp.int32, (BLK, 128), 0) & 1).astype(jnp.float32)
    odd = u - 2.0 * jnp.floor(u * 0.5)
    for h in range(2):
        wave = jnp.where(odd == float(h), u, float(DEG - 1) - u)
        c, s = cos_sin(wave * lane + 360.0 * part)
        weight = jnp.where(wave == 0.0, 1.0, 2.0)
        c, s = c * weight, s * weight
        cj, sj = cos_sin(wave * 128.0)
        for j in range(6):
            high = c.astype(jnp.bfloat16)
            hi_ref[h, pl.ds(start, BLK), 128 * j : 128 * j + 128] = high
            lo_ref[h, pl.ds(start, BLK), 128 * j : 128 * j + 128] = (c - high.astype(jnp.float32)).astype(jnp.bfloat16)
            if j < 5:
                c, s = c * cj - s * sj, s * cj + c * sj


def pack_tables(raw, wide, rows, out):
    for t in range(6):
        cols = slice(128 * t, 128 * t + 128)
        for i in range(LAT_DEV):
            wide[t, 48 * i : 48 * i + 45, :] = raw[i, :, cols].astype(jnp.float32)
            wide[t, 48 * i + 45 : 48 * i + 48, :] = jnp.zeros((3, 128), jnp.float32)
        for half in range(2):
            for s in range(3):
                for i in range(LAT_DEV):
                    got = wide[t, pl.ds(48 * i + 24 * half + s, 8, stride=3), :]
                    rows[t, pl.ds(256 * half + 3 * i + s, 8, stride=32), :] = got
            for k in (30, 31):
                rows[t, pl.ds(256 * half + k, 8, stride=32), :] = jnp.zeros((8, 128), jnp.float32)
        out[:, :, cols] = rows[t].astype(jnp.bfloat16).reshape(16, 32, 128)


def pack_coefs(raw, wide, rows, out):
    for j in range(12):
        for t, (at, size) in enumerate(((0, 128), (128, 40))):
            wide[t, 48 * j : 48 * j + 45, 0:size] = raw[j, :, at : at + size].astype(jnp.float32)
            wide[t, 48 * j + 45 : 48 * j + 48, 0:size] = jnp.zeros((3, size), jnp.float32)
    for half in range(2):
        for j in range(12):
            parts = []
            for s in range(3):
                parts.append(wide[0, pl.ds(48 * j + 24 * half + s, 8, stride=3), :])
                parts.append(wide[1, pl.ds(48 * j + 24 * half + s, 8, stride=3), :][:, 0:40])
            parts.append(jnp.zeros((8, 8), jnp.float32))
            line = jnp.concatenate(parts, axis=1)
            for t in range(4):
                rows[t, pl.ds(96 * half + j, 8, stride=12), :] = line[:, 128 * t : 128 * t + 128]
    for t in range(4):
        out[:, :, :, 128 * t : 128 * t + 128] = rows[t].astype(jnp.bfloat16).reshape(16, 3, 4, 128)


def legendre_sums(waves, table_ref, coef_ref, sums_ref, rows_ref, out_ref):
    table = table_ref[...].reshape(256, 768)
    row = lax.broadcasted_iota(jnp.int32, (768, 168), 0)
    col = lax.broadcasted_iota(jnp.int32, (768, 168), 1)
    for s in range(3):
        coefs = coef_ref[..., 168 * s : 168 * s + 168].reshape(768, 168)
        u = waves[s]
        odd = lax.rem(u, 2)
        first = DEG - u
        for h in range(2):
            low = jnp.where(odd == h, 0, first)
            high = jnp.where(odd == h, first, DEG + 1)
            kept = jnp.where((row >= low) & (row < high), coefs, jnp.zeros((), coefs.dtype))
            sums = jnp.dot(table, kept, preferred_element_type=jnp.float32)
            for e in range(2):
                sums_ref[6 * h + 2 * s + e, :, 0:CH] = sums[:, CH * e : CH * e + CH]
    lane = lax.broadcasted_iota(jnp.int32, (8, 128), 1)
    for h in range(2):
        for s in range(3):
            for e in range(2):
                lats = [sums_ref[6 * h + 2 * s + e, pl.ds(3 * i + s, 8, stride=32), :] for i in range(LAT_DEV)]
                for k in range(8):
                    i, off = divmod(CHUNK * k, CH)
                    a = lats[i] if off == 0 else pltpu.roll(lats[i], 128 - off, 1)
                    b = pltpu.roll(lats[i + 1], CH - off, 1)
                    chunk = jnp.where(lane < CH - off, a, jnp.where(lane < CHUNK, b, 0.0))
                    rows_ref[pl.ds(16 * k + 8 * h + 2 * s + e, 8, stride=128), :] = chunk
    lanes = lax.broadcasted_iota(jnp.int32, (128, 128), 1)
    for b in range(8):
        x = rows_ref[128 * b : 128 * b + 128, :]
        top = jnp.maximum(jnp.max(jnp.abs(x), axis=1, keepdims=True), 1e-37)
        level = jnp.ceil(8.0 * jnp.log2(top) + 0.01)
        x = jnp.floor(x * jnp.exp2(level * -0.125) * 32767.0 + 0.5)
        x = jnp.where(lanes == CHUNK, level, x)
        out_ref[8 * b : 8 * b + 8] = x.astype(jnp.int32).astype(jnp.int16).reshape(8, 16, 128)


def kernel(pw_s, table_hbm, coef_hbm, out_ref, table_raw, coef_raw, wide_t, rows_t, wide_c, rows_c, table_in, coef_in,
           pw_v, tab, hi, lo, table_a, table_b, coef_a, coef_b, sums_s, rows_s, send, held,
           lsem, cs, cr, ts, tr, rs, rr, fs, fr):
    lat = lax.axis_index("lat")
    ma = lax.axis_index("ma")
    y, z = lat // 8, lax.rem(lat, 8)
    along_z = [(y * 8 + lax.rem(z + d, 8), ma) for d in range(8)]
    along_y = [(lax.rem(y + d, 8) * 8 + z, ma) for d in range(8)]
    along_ma = [(lat, lax.rem(ma + d, 8)) for d in range(8)]

    get_coefs = pltpu.make_async_copy(coef_hbm, coef_raw, lsem.at[0])
    get_coefs.start()
    get_table = pltpu.make_async_copy(table_hbm, table_raw, lsem.at[1])
    get_table.start()
    barrier = pltpu.get_barrier_semaphore()
    for peers in (along_z, along_y, along_ma):
        for d in range(1, 8):
            pl.semaphore_signal(barrier, inc=1, device_id=peers[d], device_id_type=MESH)
    get_coefs.wait()
    pack_coefs(coef_raw, wide_c, rows_c, coef_in)
    pl.semaphore_wait(barrier, 21)

    def copy(src, dst, s_sem, r_sem, to):
        return pltpu.make_async_remote_copy(
            src_ref=src, dst_ref=dst, send_sem=s_sem, recv_sem=r_sem, device_id=to, device_id_type=MESH
        )

    sent = []

    def launch(c):
        c.start()
        sent.append(c)
        return c

    for d in ORDER:
        za, yb = lax.rem(z + d, 8), lax.rem(y + d, 8)
        launch(copy(coef_in.at[za], coef_a.at[y, z], cs.at[0, d], cr.at[0, d], along_z[d]))
        launch(copy(coef_in.at[8 + yb], coef_b.at[y, z], cs.at[1, d], cr.at[1, d], along_y[d]))
    coef_a[y, z] = coef_in[z]
    coef_b[y, z] = coef_in[8 + y]
    get_table.wait()
    pack_tables(table_raw, wide_t, rows_t, table_in)

    tables = []

    def send_tables(ds):
        for d in ds:
            za, yb = lax.rem(z + d, 8), lax.rem(y + d, 8)
            tables.append(launch(copy(table_in.at[za], table_a.at[z], ts.at[0, d], tr.at[0, d], along_z[d])))
            tables.append(launch(copy(table_in.at[8 + yb], table_b.at[y], ts.at[1, d], tr.at[1, d], along_y[d])))

    def basis(b):
        basis_block(b, tab, hi, lo)

    send_tables(ORDER[:2])
    wave_rows(pw_s, pw_v, tab)
    rows_s[...] = jnp.zeros_like(rows_s)

    def chunk_here(half, mine, at, peers):
        d = lax.rem(mine - at + 8, 8)
        copy(coef_in.at[0], coef_a.at[0, 0], cs.at[half, d], cr.at[half, d], peers[1]).wait_recv()

    arriving = {}
    for s in range(4):
        for k, turn in enumerate((0, 1, 3, 2)):
            pz, py = lax.rem(z // 2 + turn, 4), lax.rem(y // 2 + turn, 4)
            if s == 0:
                if turn == 0:
                    chunk_here(0, z, z + 1 - 2 * lax.rem(z, 2), along_z)
                    chunk_here(1, y, y + 1 - 2 * lax.rem(y, 2), along_y)
                else:
                    for n in range(2):
                        chunk_here(0, z, 2 * pz + n, along_z)
                        chunk_here(1, y, 2 * py + n, along_y)
            for way in range(2):
                if s == 3 and (k < 2) != (way == 0):
                    continue
                if s > 0:
                    for c in arriving.pop((s - 1, k, way)):
                        c.wait_recv()
                sign = 1 if way == 0 else 7
                by, bz = lax.rem(y + (8 - sign) * s, 8), lax.rem(z + (8 - sign) * s, 8)
                arriving[s, k, way] = []
                ref_a = coef_a.at[by, pl.ds(2 * pz, 2)]
                ref_b = coef_b.at[pl.ds(2 * py, 2), bz]
                a = copy(ref_a, ref_a, rs.at[0, way, s, k], rr.at[0, way, s, k], along_y[sign])
                b = copy(ref_b, ref_b, rs.at[1, way, s, k], rr.at[1, way, s, k], along_z[sign])
                arriving[s, k, way] += [launch(a), launch(b)]
            basis(4 * s + k)
        send_tables(ORDER[2 + 2 * s : 4 + 2 * s])
    for cs_ in arriving.values():
        for c in cs_:
            c.wait_recv()
    table_a[z] = table_in[z]
    table_b[y] = table_in[8 + y]

    sets = ((table_a, coef_a, z, along_z), (table_b, coef_b, y, along_y))
    for half, (table, coef, mine, peers) in enumerate(sets):
        for c in tables[half::2]:
            c.wait_recv()
        at = ma * 45 + half * 24 + mine * 3
        waves = [pw_s[jnp.minimum(at + s, 359)] for s in range(3)]
        legendre_sums(waves, table, coef, sums_s, rows_s, send.at[half])
        for d in ORDER + (0,):
            to = lax.rem(mine + d, 8)

            def step(n, _, d=d, to=to, half=half, mine=mine, peers=peers):
                m2 = lax.rem(ma + n, 8)
                copy(
                    send.at[half, to * 8 + m2], held.at[half, ma * 8 + mine], fs.at[half], fr.at[half], (peers[d][0], m2)
                ).start()
                return 0

            lax.fori_loop(0 if d else 1, 8, step, 0)
        held[half, ma * 8 + mine] = send[half, mine * 8 + ma]

    dims = (((0,), (0,)), ((), ()))
    totals = [None, None]
    for half in range(2):
        most = pl.ds(0, 63)
        copy(send.at[half, most], held.at[half, most], fs.at[half], fr.at[half], along_z[1]).wait_recv()
        for h in range(2):
            x = held[half].astype(jnp.int32).astype(jnp.float32)[:, 8 * h : 8 * h + 8, :].reshape(512, 128)
            x = x * (jnp.exp2(x[:, CHUNK : CHUNK + 1] * 0.125) * (1.0 / 32767.0))
            high = x.astype(jnp.bfloat16)
            low = (x - high.astype(jnp.float32)).astype(jnp.bfloat16)
            b_hi, b_lo = hi[h, 512 * half : 512 * half + 512, :], lo[h, 512 * half : 512 * half + 512, :]
            total = lax.dot_general(high, b_hi, dims, preferred_element_type=jnp.float32)
            total += lax.dot_general(low, b_hi, dims, preferred_element_type=jnp.float32)
            total += lax.dot_general(high, b_lo, dims, preferred_element_type=jnp.float32)
            totals[h] = total if half == 0 else totals[h] + total
    out_ref[:, 0:HALF] = (totals[0] + totals[1])[:CHUNK, :HALF]
    out_ref[:, HALF:LON] = (totals[0] - totals[1])[:CHUNK, :HALF]
    for c in sent:
        c.wait_send()
    for half in range(2):
        copy(send.at[half, most], held.at[half, most], fs.at[half], fr.at[half], along_z[1]).wait_send()


def body(pair_wave, legendre, coefs):
    vmem, hbm = pl.BlockSpec(memory_space=pltpu.VMEM), pl.BlockSpec(memory_space=pl.ANY)
    bf16, f32, dma = jnp.bfloat16, jnp.float32, pltpu.SemaphoreType.DMA
    return pl.pallas_call(
        kernel,
        out_shape=jax.ShapeDtypeStruct((CHUNK, LON), f32),
        in_specs=[pl.BlockSpec(memory_space=pltpu.SMEM), hbm, hbm],
        out_specs=vmem,
        scratch_shapes=[
            pltpu.VMEM((LAT_DEV, 45, 768), bf16),
            pltpu.VMEM((12, 45, 168), bf16),
            pltpu.VMEM((6, 480, 128), f32),
            pltpu.VMEM((6, 512, 128), f32),
            pltpu.VMEM((2, 576, 128), f32),
            pltpu.VMEM((4, 192, 128), f32),
            pltpu.VMEM((16, 32, 768), bf16),
            pltpu.VMEM((16, 3, 4, 512), bf16),
            pltpu.VMEM((8, 384), jnp.int32),
            pltpu.VMEM((ROWS, 128), f32),
            pltpu.VMEM((2, ROWS, 768), bf16),
            pltpu.VMEM((2, ROWS, 768), bf16),
            pltpu.VMEM((8, 32, 768), bf16),
            pltpu.VMEM((8, 32, 768), bf16),
            pltpu.VMEM((8, 8, 3, 4, 512), bf16),
            pltpu.VMEM((8, 8, 3, 4, 512), bf16),
            pltpu.VMEM((12, 256, 128), f32),
            pltpu.VMEM((1024, 128), f32),
            pltpu.VMEM((2, 64, 16, 128), jnp.int16),
            pltpu.VMEM((2, 64, 16, 128), jnp.int16),
            dma((2,)),
            dma((2, 8)), dma((2, 8)), dma((2, 8)), dma((2, 8)),
            dma((2, 2, 4, 4)), dma((2, 2, 4, 4)), dma((2,)), dma((2,)),
        ],
        compiler_params=pltpu.CompilerParams(
            collective_id=0, has_side_effects=True, vmem_limit_bytes=60 * 2**20
        ),
    )(pair_wave, jnp.transpose(legendre, (1, 0, 2)), jnp.transpose(coefs, (1, 0, 2)))


def solution(mesh):
    placed = (P(), P("ma", "lat", None), P("ma", "lat", None))
    return jax.shard_map(
        body, mesh=mesh, in_specs=placed, out_specs=P(("lat", "ma"), None), check_vma=False
    )
```

```python
import math

import jax
import jax.numpy as jnp
from jax import lax
from jax.experimental import pallas as pl
from jax.experimental.pallas import tpu as pltpu
from jax.sharding import PartitionSpec as P

DEG = 720
LON = 1440
HALF = LON // 2
CH = 84
LAT_DEV = 10
CHUNK = LAT_DEV * CH // 8
MESH = pl.DeviceIdType.MESH
ORDER = (4, 3, 5, 2, 6, 1, 7)
ROWS = 1024
SENDS = (((4, 3), (5, 2), (6, 1), (7,), ()), ((4, 3), (5, 2), (6, 1), (7,), ()))
BLK = 64


def wave_rows(pw_s, pw_v, tab_ref):
    lane = lax.broadcasted_iota(jnp.int32, (8, 128), 1)
    for t in range(3):

        def gather(n, v):
            for k in range(8):
                at = t * 128 + n * 8 + k
                v = jnp.where(lane == n * 8 + k, pw_s[jnp.minimum(at, 359)], v)
            return v

        pw_v[:, 128 * t : 128 * t + 128] = lax.fori_loop(0, 16, gather, jnp.zeros((8, 128), jnp.int32))
    pw = pw_v[0:1, :]
    half = jnp.broadcast_to((pw >> 1).astype(jnp.float32).astype(jnp.bfloat16), (128, 384))
    low = jnp.broadcast_to((pw & 1).astype(jnp.float32).astype(jnp.bfloat16), (128, 384))

    def step(b, _):
        row = lax.broadcasted_iota(jnp.int32, (256, 384), 0) + b * 256
        col = lax.broadcasted_iota(jnp.int32, (256, 384), 1)
        slot = jnp.where(((row >> 8) & 1) == 1, 2, (row & 3) >> 1)
        slot = 24 * (row >> 9) + 3 * ((row >> 2) & 7) + slot
        slot = ((row >> 5) & 7) * 45 + jnp.where(slot < 45, slot, 0)
        pick = jnp.where(col == slot, 1.0, 0.0).astype(jnp.bfloat16)
        dims = (((1,), (1,)), ((), ()))
        hi = lax.dot_general(pick, half, dims, preferred_element_type=jnp.float32)
        lo = lax.dot_general(pick, low, dims, preferred_element_type=jnp.float32)
        tab_ref[pl.ds(pl.multiple_of(b * 256, 256), 256), :] = 2.0 * hi + lo
        return 0

    lax.fori_loop(0, ROWS // 256, step, 0)


def cos_sin(phase):
    turns = jnp.floor(phase * (1.0 / LON))
    t = (phase - turns * LON - HALF) * (2.0 * math.pi / LON / 4.0)
    q = t * t
    s = t * (1.0 + q * (-1.0 / 6 + q * (1.0 / 120 + q * (-1.0 / 5040 + q * (1.0 / 362880)))))
    c = 1.0 + q * (-0.5 + q * (1.0 / 24 + q * (-1.0 / 720 + q * (1.0 / 40320 - q * (1.0 / 3628800)))))
    s, c = 2.0 * s * c, 1.0 - 2.0 * s * s
    s, c = 2.0 * s * c, 1.0 - 2.0 * s * s
    return -c, -s


def basis_block(b, tab_ref, hi_ref, lo_ref):
    start = b * BLK
    u = tab_ref[pl.ds(start, BLK), :]
    lane = lax.broadcasted_iota(jnp.int32, (BLK, 128), 1).astype(jnp.float32)
    part = (lax.broadcasted_iota(jnp.int32, (BLK, 128), 0) & 1).astype(jnp.float32)
    odd = u - 2.0 * jnp.floor(u * 0.5)
    for h in range(2):
        wave = jnp.where(odd == float(h), u, float(DEG - 1) - u)
        c, s = cos_sin(wave * lane + 360.0 * part)
        weight = jnp.where(wave == 0.0, 1.0, 2.0)
        if b % 8 >= 4:
            weight = jnp.where((lax.broadcasted_iota(jnp.int32, (BLK, 128), 0) >> 1) & 1 == h, weight, 0.0)
        c, s = c * weight, s * weight
        cj, sj = cos_sin(wave * 128.0)
        for j in range(6):
            high = c.astype(jnp.bfloat16)
            hi_ref[h, pl.ds(start, BLK), 128 * j : 128 * j + 128] = high
            lo_ref[h, pl.ds(start, BLK), 128 * j : 128 * j + 128] = (c - high.astype(jnp.float32)).astype(jnp.bfloat16)
            if j < 5:
                c, s = c * cj - s * sj, s * cj + c * sj


def pack_tables(raw, wide, rows, out):
    for t in range(6):
        cols = slice(128 * t, 128 * t + 128)
        for i in range(LAT_DEV):
            wide[t, 48 * i : 48 * i + 45, :] = raw[i, :, cols].astype(jnp.float32)
            wide[t, 48 * i + 45 : 48 * i + 48, :] = jnp.zeros((3, 128), jnp.float32)
        for half in range(2):
            for s in range(3):
                for i in range(LAT_DEV):
                    got = wide[t, pl.ds(48 * i + 24 * half + s, 8, stride=3), :]
                    rows[t, pl.ds(256 * half + 3 * i + s, 8, stride=32), :] = got
            for k in (30, 31):
                rows[t, pl.ds(256 * half + k, 8, stride=32), :] = jnp.zeros((8, 128), jnp.float32)
        out[:, :, cols] = rows[t].astype(jnp.bfloat16).reshape(16, 32, 128)


def pack_coefs(raw, wide, rows, out):
    for j in range(12):
        for t, (at, size) in enumerate(((0, 128), (128, 40))):
            wide[t, 48 * j : 48 * j + 45, 0:size] = raw[j, :, at : at + size].astype(jnp.float32)
            wide[t, 48 * j + 45 : 48 * j + 48, 0:size] = jnp.zeros((3, size), jnp.float32)
    for half in range(2):
        for j in range(12):
            parts = []
            for s in range(3):
                parts.append(wide[0, pl.ds(48 * j + 24 * half + s, 8, stride=3), :])
                parts.append(wide[1, pl.ds(48 * j + 24 * half + s, 8, stride=3), :][:, 0:40])
            parts.append(jnp.zeros((8, 8), jnp.float32))
            line = jnp.concatenate(parts, axis=1)
            for t in range(4):
                rows[t, pl.ds(96 * half + j, 8, stride=12), :] = line[:, 128 * t : 128 * t + 128]
    for t in range(4):
        out[:, :, :, 128 * t : 128 * t + 128] = rows[t].astype(jnp.bfloat16).reshape(16, 3, 4, 128)


def legendre_sums(waves, table_ref, coef_ref, sums_ref, rows_ref):
    table = table_ref[...].reshape(256, 768)
    coefs = coef_ref[...].reshape(768, 512)
    row = lax.broadcasted_iota(jnp.int32, (768, 512), 0)
    slot = lax.broadcasted_iota(jnp.int32, (1, 512), 1)

    def by_slot(values):
        return jnp.where(slot < 168, values[0], jnp.where(slot < 336, values[1], values[2]))

    for h in range(2):
        low = by_slot([jnp.where(lax.rem(u, 2) == h, 0, DEG - u) for u in waves])
        high = by_slot([jnp.where(lax.rem(u, 2) == h, DEG - u, DEG + 1) for u in waves])
        kept = jnp.where((row >= low) & (row < high), coefs, jnp.zeros((), coefs.dtype))
        sums = jnp.dot(table, kept, preferred_element_type=jnp.float32)
        for t in range(6):
            sums_ref[6 * h + t, :, 0:CH] = sums[:, CH * t : CH * t + CH]
    lane = lax.broadcasted_iota(jnp.int32, (8, 128), 1)
    for h in range(2):
        for s in range(3):
            for e in range(2):
                lats = [sums_ref[6 * h + 2 * s + e, pl.ds(3 * i + s, 8, stride=32), :] for i in range(LAT_DEV)]
                for k in range(8):
                    i, off = divmod(CHUNK * k, CH)
                    a = lats[i] if off == 0 else pltpu.roll(lats[i], 128 - off, 1)
                    b = pltpu.roll(lats[i + 1], CH - off, 1)
                    chunk = jnp.where(lane < CH - off, a, jnp.where(lane < CHUNK, b, 0.0))
                    at = e + (2 * s if h == 0 else 6 if s == 2 else 8 + 2 * s)
                    rows_ref[pl.ds(12 * k + at, 8, stride=96), :] = chunk

def packed(rows_ref, source):
    lanes = lax.broadcasted_iota(jnp.int32, (96, 128), 1)
    x = rows_ref[pl.ds(pl.multiple_of(96 * source, 96), 96), :]
    top = jnp.maximum(jnp.max(jnp.abs(x), axis=1, keepdims=True), 1e-37)
    level = jnp.ceil(8.0 * jnp.log2(top) + 0.01)
    x = jnp.floor(x * jnp.exp2(level * -0.125) * 32767.0 + 0.5)
    x = jnp.where(lanes == CHUNK, level, x)
    return x.astype(jnp.int32).astype(jnp.int16).reshape(8, 3, 4, 128)


def kernel(pw_s, table_hbm, coef_hbm, out_ref, table_raw, coef_raw, wide_t, rows_t, wide_c, rows_c, table_in, coef_in,
           pw_v, tab, hi, lo, table_a, table_b, coef_a, coef_b, sums_s, rows_s, send, held,
           lsem, cs, cr, ts, tr, rs, rr, fs, fr):
    lat = lax.axis_index("lat")
    ma = lax.axis_index("ma")
    y, z = lat // 8, lax.rem(lat, 8)
    along_z = [(y * 8 + lax.rem(z + d, 8), ma) for d in range(8)]
    along_y = [(lax.rem(y + d, 8) * 8 + z, ma) for d in range(8)]
    along_ma = [(lat, lax.rem(ma + d, 8)) for d in range(8)]

    get_coefs = pltpu.make_async_copy(coef_hbm, coef_raw, lsem.at[0])
    get_coefs.start()
    get_table = pltpu.make_async_copy(table_hbm, table_raw, lsem.at[1])
    get_table.start()
    barrier = pltpu.get_barrier_semaphore()
    for peers in (along_z, along_y, along_ma):
        for d in range(1, 8):
            pl.semaphore_signal(barrier, inc=1, device_id=peers[d], device_id_type=MESH)
    get_coefs.wait()
    pack_coefs(coef_raw, wide_c, rows_c, coef_in)
    pl.semaphore_wait(barrier, 21)

    def copy(src, dst, s_sem, r_sem, to):
        return pltpu.make_async_remote_copy(
            src_ref=src, dst_ref=dst, send_sem=s_sem, recv_sem=r_sem, device_id=to, device_id_type=MESH
        )

    sent = []

    def launch(c):
        c.start()
        sent.append(c)
        return c

    for d in ORDER:
        za, yb = lax.rem(z + d, 8), lax.rem(y + d, 8)
        launch(copy(coef_in.at[za], coef_a.at[y, z], cs.at[0, d], cr.at[0, d], along_z[d]))
        launch(copy(coef_in.at[8 + yb], coef_b.at[y, z], cs.at[1, d], cr.at[1, d], along_y[d]))
    coef_a[y, z] = coef_in[z]
    coef_b[y, z] = coef_in[8 + y]
    get_table.wait()
    pack_tables(table_raw, wide_t, rows_t, table_in)

    tables = ([], [])

    def send_tables(turn):
        for half, (mine, table, peers) in enumerate(((z, table_a, along_z), (y, table_b, along_y))):
            for d in SENDS[half][turn]:
                to = lax.rem(mine + d, 8)
                tables[half].append(
                    launch(copy(table_in.at[8 * half + to], table.at[mine], ts.at[half, d], tr.at[half, d], peers[d]))
                )

    def basis(b):
        basis_block(b, tab, hi, lo)

    send_tables(0)
    wave_rows(pw_s, pw_v, tab)

    def chunk_here(half, mine, at, peers):
        d = lax.rem(mine - at + 8, 8)
        copy(coef_in.at[0], coef_a.at[0, 0], cs.at[half, d], cr.at[half, d], peers[1]).wait_recv()

    arriving = {}
    for s in range(4):
        for k, turn in enumerate((0, 1, 3, 2)):
            pz, py = lax.rem(z // 2 + turn, 4), lax.rem(y // 2 + turn, 4)
            for half, (mine, peers) in enumerate(((z, along_z), (y, along_y))):
                if s == 0:
                    if turn == 0:
                        chunk_here(half, mine, mine + 1 - 2 * lax.rem(mine, 2), peers)
                    else:
                        for n in range(2):
                            chunk_here(half, mine, 2 * (py if half else pz) + n, peers)
                for way in range(2):
                    if s == 3 and (k < 2) != (way == 0):
                        continue
                    if s > 0:
                        arriving.pop((s - 1, k, way, half)).wait_recv()
                    sign = 1 if way == 0 else 7
                    back = (8 - sign) * s
                    if half == 0:
                        ref, to = coef_a.at[lax.rem(y + back, 8), pl.ds(2 * pz, 2)], along_y[sign]
                    else:
                        ref, to = coef_b.at[pl.ds(2 * py, 2), lax.rem(z + back, 8)], along_z[sign]
                    arriving[s, k, way, half] = launch(
                        copy(ref, ref, rs.at[half, way, s, k], rr.at[half, way, s, k], to)
                    )
            basis(4 * s + k)
        send_tables(1 + s)
    table_a[z] = table_in[z]
    table_b[y] = table_in[8 + y]

    sets = ((table_a, coef_a, z, along_z), (table_b, coef_b, y, along_y))
    for half, (table, coef, mine, peers) in enumerate(sets):
        for key, c in arriving.items():
            if key[3] == half:
                c.wait_recv()
        for c in tables[half]:
            c.wait_recv()
        at = ma * 45 + half * 24 + mine * 3
        waves = [pw_s[jnp.minimum(at + s, 359)] for s in range(3)]
        legendre_sums(waves, table, coef, sums_s, rows_s)
        for d in ORDER + (0,):
            to = lax.rem(mine + d, 8)
            send[half, pl.ds(pl.multiple_of(8 * to, 8), 8)] = packed(rows_s, to)

            def step(n, _, d=d, to=to, half=half, mine=mine, peers=peers):
                m2 = lax.rem(ma + n, 8)
                copy(
                    send.at[half, to * 8 + m2], held.at[half, ma * 8 + mine], fs.at[half], fr.at[half], (peers[d][0], m2)
                ).start()
                return 0

            lax.fori_loop(0 if d else 1, 8, step, 0)
        held[half, ma * 8 + mine] = send[half, mine * 8 + ma]

    dims = (((0,), (0,)), ((), ()))
    totals = [None, None]
    for half in range(2):
        most = pl.ds(0, 63)
        copy(send.at[half, most], held.at[half, most], fs.at[half], fr.at[half], along_z[1]).wait_recv()
        for h in range(2):
            own, both = (held[half, :, t].astype(jnp.int32).astype(jnp.float32).reshape(256, 128) for t in (2 * h, 1))
            x = jnp.concatenate([own, both], axis=0)
            x = x * (jnp.exp2(x[:, CHUNK : CHUNK + 1] * 0.125) * (1.0 / 32767.0))
            high = x.astype(jnp.bfloat16)
            low = (x - high.astype(jnp.float32)).astype(jnp.bfloat16)
            b_hi, b_lo = hi[h, 512 * half : 512 * half + 512, :], lo[h, 512 * half : 512 * half + 512, :]
            total = lax.dot_general(high, b_hi, dims, preferred_element_type=jnp.float32)
            total += lax.dot_general(low, b_hi, dims, preferred_element_type=jnp.float32)
            total += lax.dot_general(high, b_lo, dims, preferred_element_type=jnp.float32)
            totals[h] = total if half == 0 else totals[h] + total
    out_ref[:, 0:HALF] = (totals[0] + totals[1])[:CHUNK, :HALF]
    out_ref[:, HALF:LON] = (totals[0] - totals[1])[:CHUNK, :HALF]
    for c in sent:
        c.wait_send()
    for half in range(2):
        copy(send.at[half, most], held.at[half, most], fs.at[half], fr.at[half], along_z[1]).wait_send()


def body(pair_wave, legendre, coefs):
    vmem, hbm = pl.BlockSpec(memory_space=pltpu.VMEM), pl.BlockSpec(memory_space=pl.ANY)
    bf16, f32, dma = jnp.bfloat16, jnp.float32, pltpu.SemaphoreType.DMA
    return pl.pallas_call(
        kernel,
        out_shape=jax.ShapeDtypeStruct((CHUNK, LON), f32),
        in_specs=[pl.BlockSpec(memory_space=pltpu.SMEM), hbm, hbm],
        out_specs=vmem,
        scratch_shapes=[
            pltpu.VMEM((LAT_DEV, 45, 768), bf16),
            pltpu.VMEM((12, 45, 168), bf16),
            pltpu.VMEM((6, 480, 128), f32),
            pltpu.VMEM((6, 512, 128), f32),
            pltpu.VMEM((2, 576, 128), f32),
            pltpu.VMEM((4, 192, 128), f32),
            pltpu.VMEM((16, 32, 768), bf16),
            pltpu.VMEM((16, 3, 4, 512), bf16),
            pltpu.VMEM((8, 384), jnp.int32),
            pltpu.VMEM((ROWS, 128), f32),
            pltpu.VMEM((2, ROWS, 768), bf16),
            pltpu.VMEM((2, ROWS, 768), bf16),
            pltpu.VMEM((8, 32, 768), bf16),
            pltpu.VMEM((8, 32, 768), bf16),
            pltpu.VMEM((8, 8, 3, 4, 512), bf16),
            pltpu.VMEM((8, 8, 3, 4, 512), bf16),
            pltpu.VMEM((12, 256, 128), f32),
            pltpu.VMEM((768, 128), f32),
            pltpu.VMEM((2, 64, 3, 4, 128), jnp.int16),
            pltpu.VMEM((2, 64, 3, 4, 128), jnp.int16),
            dma((2,)),
            dma((2, 8)), dma((2, 8)), dma((2, 8)), dma((2, 8)),
            dma((2, 2, 4, 4)), dma((2, 2, 4, 4)), dma((2,)), dma((2,)),
        ],
        compiler_params=pltpu.CompilerParams(
            collective_id=0, has_side_effects=True, vmem_limit_bytes=60 * 2**20
        ),
    )(pair_wave, jnp.transpose(legendre, (1, 0, 2)), jnp.transpose(coefs, (1, 0, 2)))


def solution(mesh):
    placed = (P(), P("ma", "lat", None), P("ma", "lat", None))
    return jax.shard_map(
        body, mesh=mesh, in_specs=placed, out_specs=P(("lat", "ma"), None), check_vma=False
    )
```

```python
import math

import jax
import jax.numpy as jnp
from jax import lax
from jax.experimental import pallas as pl
from jax.experimental.pallas import tpu as pltpu
from jax.sharding import PartitionSpec as P

DEG = 720
LON = 1440
HALF = LON // 2
CH = 84
LAT_DEV = 10
CHUNK = LAT_DEV * CH // 8
MESH = pl.DeviceIdType.MESH
ORDER = (4, 3, 5, 2, 6, 1, 7)
ROWS = 1024
SENDS = (((4, 3), (5, 2), (6, 1), (7,), ()), ((4, 3), (5, 2), (6, 1), (7,), ()))
BLK = 64


def wave_rows(pw_s, pw_v, tab_ref):
    lane = lax.broadcasted_iota(jnp.int32, (8, 128), 1)
    for t in range(3):

        def gather(n, v):
            for k in range(8):
                at = t * 128 + n * 8 + k
                v = jnp.where(lane == n * 8 + k, pw_s[jnp.minimum(at, 359)], v)
            return v

        pw_v[:, 128 * t : 128 * t + 128] = lax.fori_loop(0, 16, gather, jnp.zeros((8, 128), jnp.int32))
    pw = pw_v[0:1, :]
    half = jnp.broadcast_to((pw >> 1).astype(jnp.float32).astype(jnp.bfloat16), (128, 384))
    low = jnp.broadcast_to((pw & 1).astype(jnp.float32).astype(jnp.bfloat16), (128, 384))

    def step(b, _):
        row = lax.broadcasted_iota(jnp.int32, (256, 384), 0) + b * 256
        col = lax.broadcasted_iota(jnp.int32, (256, 384), 1)
        slot = jnp.where(((row >> 8) & 1) == 1, 2, (row & 3) >> 1)
        slot = 24 * (row >> 9) + 3 * ((row >> 2) & 7) + slot
        slot = ((row >> 5) & 7) * 45 + jnp.where(slot < 45, slot, 0)
        pick = jnp.where(col == slot, 1.0, 0.0).astype(jnp.bfloat16)
        dims = (((1,), (1,)), ((), ()))
        hi = lax.dot_general(pick, half, dims, preferred_element_type=jnp.float32)
        lo = lax.dot_general(pick, low, dims, preferred_element_type=jnp.float32)
        tab_ref[pl.ds(pl.multiple_of(b * 256, 256), 256), :] = 2.0 * hi + lo
        return 0

    lax.fori_loop(0, ROWS // 256, step, 0)


def cos_sin(phase):
    turns = jnp.floor(phase * (1.0 / LON))
    t = (phase - turns * LON - HALF) * (2.0 * math.pi / LON / 4.0)
    q = t * t
    s = t * (1.0 + q * (-1.0 / 6 + q * (1.0 / 120 + q * (-1.0 / 5040 + q * (1.0 / 362880)))))
    c = 1.0 + q * (-0.5 + q * (1.0 / 24 + q * (-1.0 / 720 + q * (1.0 / 40320 - q * (1.0 / 3628800)))))
    s, c = 2.0 * s * c, 1.0 - 2.0 * s * s
    s, c = 2.0 * s * c, 1.0 - 2.0 * s * s
    return -c, -s


def basis_block(b, tab_ref, hi_ref, lo_ref):
    start = b * BLK
    u = tab_ref[pl.ds(start, BLK), :]
    lane = lax.broadcasted_iota(jnp.int32, (BLK, 128), 1).astype(jnp.float32)
    part = (lax.broadcasted_iota(jnp.int32, (BLK, 128), 0) & 1).astype(jnp.float32)
    odd = u - 2.0 * jnp.floor(u * 0.5)
    for h in range(2):
        wave = jnp.where(odd == float(h), u, float(DEG - 1) - u)
        c, s = cos_sin(wave * lane + 360.0 * part)
        weight = jnp.where(wave == 0.0, 1.0, 2.0)
        if b % 8 >= 4:
            weight = jnp.where((lax.broadcasted_iota(jnp.int32, (BLK, 128), 0) >> 1) & 1 == h, weight, 0.0)
        c, s = c * weight, s * weight
        cj, sj = cos_sin(wave * 128.0)
        for j in range(6):
            high = c.astype(jnp.bfloat16)
            hi_ref[h, pl.ds(start, BLK), 128 * j : 128 * j + 128] = high
            lo_ref[h, pl.ds(start, BLK), 128 * j : 128 * j + 128] = (c - high.astype(jnp.float32)).astype(jnp.bfloat16)
            if j < 5:
                c, s = c * cj - s * sj, s * cj + c * sj


def pack_tables(raw, wide, rows, out):
    for t in range(6):
        cols = slice(128 * t, 128 * t + 128)
        for i in range(LAT_DEV):
            wide[t, 48 * i : 48 * i + 45, :] = raw[i, :, cols].astype(jnp.float32)
            wide[t, 48 * i + 45 : 48 * i + 48, :] = jnp.zeros((3, 128), jnp.float32)
        for half in range(2):
            for s in range(3):
                for i in range(LAT_DEV):
                    got = wide[t, pl.ds(48 * i + 24 * half + s, 8, stride=3), :]
                    rows[t, pl.ds(256 * half + 3 * i + s, 8, stride=32), :] = got
            for k in (30, 31):
                rows[t, pl.ds(256 * half + k, 8, stride=32), :] = jnp.zeros((8, 128), jnp.float32)
        out[:, :, cols] = rows[t].astype(jnp.bfloat16).reshape(16, 32, 128)


def pack_coefs(raw, wide, rows, out):
    for j in range(12):
        for t, (at, size) in enumerate(((0, 128), (128, 40))):
            wide[t, 48 * j : 48 * j + 45, 0:size] = raw[j, :, at : at + size].astype(jnp.float32)
            wide[t, 48 * j + 45 : 48 * j + 48, 0:size] = jnp.zeros((3, size), jnp.float32)
    for half in range(2):
        for j in range(12):
            parts = []
            for s in range(3):
                parts.append(wide[0, pl.ds(48 * j + 24 * half + s, 8, stride=3), :])
                parts.append(wide[1, pl.ds(48 * j + 24 * half + s, 8, stride=3), :][:, 0:40])
            parts.append(jnp.zeros((8, 8), jnp.float32))
            line = jnp.concatenate(parts, axis=1)
            for t in range(4):
                rows[t, pl.ds(96 * half + j, 8, stride=12), :] = line[:, 128 * t : 128 * t + 128]
    for t in range(4):
        out[:, :, :, 128 * t : 128 * t + 128] = rows[t].astype(jnp.bfloat16).reshape(16, 3, 4, 128)


def legendre_sums(waves, table_ref, coef_ref, sums_ref, rows_ref):
    table = table_ref[...].reshape(256, 768)
    coefs = coef_ref[...].reshape(768, 512)
    row = lax.broadcasted_iota(jnp.int32, (768, 512), 0)
    slot = lax.broadcasted_iota(jnp.int32, (1, 512), 1)

    def by_slot(values):
        return jnp.where(slot < 168, values[0], jnp.where(slot < 336, values[1], values[2]))

    for h in range(2):
        low = by_slot([jnp.where(lax.rem(u, 2) == h, 0, DEG - u) for u in waves])
        high = by_slot([jnp.where(lax.rem(u, 2) == h, DEG - u, DEG + 1) for u in waves])
        kept = jnp.where((row >= low) & (row < high), coefs, jnp.zeros((), coefs.dtype))
        sums = jnp.dot(table, kept, preferred_element_type=jnp.float32)
        for t in range(6):
            sums_ref[6 * h + t, :, 0:CH] = sums[:, CH * t : CH * t + CH]
    lane = lax.broadcasted_iota(jnp.int32, (8, 128), 1)
    for h in range(2):
        for s in range(3):
            for e in range(2):
                lats = [sums_ref[6 * h + 2 * s + e, pl.ds(3 * i + s, 8, stride=32), :] for i in range(LAT_DEV)]
                for k in range(8):
                    i, off = divmod(CHUNK * k, CH)
                    a = lats[i] if off == 0 else pltpu.roll(lats[i], 128 - off, 1)
                    b = pltpu.roll(lats[i + 1], CH - off, 1)
                    chunk = jnp.where(lane < CH - off, a, jnp.where(lane < CHUNK, b, 0.0))
                    at = e + (2 * s if h == 0 else 6 if s == 2 else 8 + 2 * s)
                    rows_ref[pl.ds(12 * k + at, 8, stride=96), :] = chunk

def packed(rows_ref, source):
    lanes = lax.broadcasted_iota(jnp.int32, (96, 128), 1)
    x = rows_ref[pl.ds(pl.multiple_of(96 * source, 96), 96), :]
    top = jnp.maximum(jnp.max(jnp.abs(x), axis=1, keepdims=True), 1e-37)
    level = jnp.ceil(8.0 * jnp.log2(top) + 0.01)
    x = jnp.floor(x * jnp.exp2(level * -0.125) * 32767.0 + 0.5)
    x = jnp.where(lanes == CHUNK, level, x)
    return x.astype(jnp.int32).astype(jnp.int16).reshape(8, 3, 4, 128)


def kernel(pw_s, table_hbm, coef_hbm, out_ref, table_raw, coef_raw, wide_t, rows_t, wide_c, rows_c, table_in, coef_in,
           pw_v, tab, hi, lo, table_a, table_b, coef_a, coef_b, sums_s, rows_s, send, held,
           lsem, cs, cr, ts, tr, rs, rr, fs, fr):
    lat = lax.axis_index("lat")
    ma = lax.axis_index("ma")
    y, z = lat // 8, lax.rem(lat, 8)
    along_z = [(y * 8 + lax.rem(z + d, 8), ma) for d in range(8)]
    along_y = [(lax.rem(y + d, 8) * 8 + z, ma) for d in range(8)]
    along_ma = [(lat, lax.rem(ma + d, 8)) for d in range(8)]

    get_coefs = pltpu.make_async_copy(coef_hbm, coef_raw, lsem.at[0])
    get_coefs.start()
    get_table = pltpu.make_async_copy(table_hbm, table_raw, lsem.at[1])
    get_table.start()
    barrier = pltpu.get_barrier_semaphore()
    for peers in (along_z, along_y, along_ma):
        for d in range(1, 8):
            pl.semaphore_signal(barrier, inc=1, device_id=peers[d], device_id_type=MESH)
    get_coefs.wait()
    pack_coefs(coef_raw, wide_c, rows_c, coef_in)
    pl.semaphore_wait(barrier, 21)

    def copy(src, dst, s_sem, r_sem, to):
        return pltpu.make_async_remote_copy(
            src_ref=src, dst_ref=dst, send_sem=s_sem, recv_sem=r_sem, device_id=to, device_id_type=MESH
        )

    sent = []

    def launch(c):
        c.start()
        sent.append(c)
        return c

    for d in ORDER:
        za, yb = lax.rem(z + d, 8), lax.rem(y + d, 8)
        launch(copy(coef_in.at[za], coef_a.at[y, z], cs.at[0, d], cr.at[0, d], along_z[d]))
        launch(copy(coef_in.at[8 + yb], coef_b.at[y, z], cs.at[1, d], cr.at[1, d], along_y[d]))
    coef_a[y, z] = coef_in[z]
    coef_b[y, z] = coef_in[8 + y]
    get_table.wait()
    pack_tables(table_raw, wide_t, rows_t, table_in)

    tables = ([], [])

    def send_tables(turn):
        for half, (mine, table, peers) in enumerate(((z, table_a, along_z), (y, table_b, along_y))):
            for d in SENDS[half][turn]:
                to = lax.rem(mine + d, 8)
                tables[half].append(
                    launch(copy(table_in.at[8 * half + to], table.at[mine], ts.at[half, d], tr.at[half, d], peers[d]))
                )

    def basis(b):
        basis_block(b, tab, hi, lo)

    send_tables(0)
    wave_rows(pw_s, pw_v, tab)

    def chunk_here(half, mine, at, peers):
        d = lax.rem(mine - at + 8, 8)
        copy(coef_in.at[0], coef_a.at[0, 0], cs.at[half, d], cr.at[half, d], peers[1]).wait_recv()

    arriving = {}
    for s in range(4):
        for k, turn in enumerate((0, 1, 3, 2)):
            pz, py = lax.rem(z // 2 + turn, 4), lax.rem(y // 2 + turn, 4)
            for half, (mine, peers) in enumerate(((z, along_z), (y, along_y))):
                if s == 0:
                    if turn == 0:
                        chunk_here(half, mine, mine + 1 - 2 * lax.rem(mine, 2), peers)
                    else:
                        for n in range(2):
                            chunk_here(half, mine, 2 * (py if half else pz) + n, peers)
                for way in range(2):
                    if s == 3 and (k < 2) != (way == 0):
                        continue
                    if s > 0:
                        arriving.pop((s - 1, k, way, half)).wait_recv()
                    sign = 1 if way == 0 else 7
                    back = (8 - sign) * s
                    if half == 0:
                        ref, to = coef_a.at[lax.rem(y + back, 8), pl.ds(2 * pz, 2)], along_y[sign]
                    else:
                        ref, to = coef_b.at[pl.ds(2 * py, 2), lax.rem(z + back, 8)], along_z[sign]
                    arriving[s, k, way, half] = launch(
                        copy(ref, ref, rs.at[half, way, s, k], rr.at[half, way, s, k], to)
                    )
            basis(4 * s + k)
        send_tables(1 + s)
    table_a[z] = table_in[z]
    table_b[y] = table_in[8 + y]

    sets = ((table_a, coef_a, z, along_z), (table_b, coef_b, y, along_y))
    for half, (table, coef, mine, peers) in enumerate(sets):
        for key, c in arriving.items():
            if key[3] == half:
                c.wait_recv()
        for c in tables[half]:
            c.wait_recv()
        at = ma * 45 + half * 24 + mine * 3
        waves = [pw_s[jnp.minimum(at + s, 359)] for s in range(3)]
        legendre_sums(waves, table, coef, sums_s, rows_s)
        for d in ORDER + (0,):
            to = lax.rem(mine + d, 8)
            send[half, pl.ds(pl.multiple_of(8 * to, 8), 8)] = packed(rows_s, to)

        def out(n, ds, half=half, mine=mine, peers=peers):
            m2 = lax.rem(ma + n, 8)
            for d in ds:
                to = lax.rem(mine + d, 8)
                copy(
                    send.at[half, to * 8 + m2], held.at[half, ma * 8 + mine], fs.at[half], fr.at[half], (peers[d][0], m2)
                ).start()
            return 0

        lax.fori_loop(1, 8, lambda n, _, out=out: out(n, ORDER + (0,)), 0)
        out(0, ORDER)
        held[half, ma * 8 + mine] = send[half, mine * 8 + ma]

    dims = (((0,), (0,)), ((), ()))
    totals = [None, None]
    for half in range(2):
        most = pl.ds(0, 63)
        copy(send.at[half, most], held.at[half, most], fs.at[half], fr.at[half], along_z[1]).wait_recv()
        for h in range(2):
            own, both = (held[half, :, t].astype(jnp.int32).astype(jnp.float32).reshape(256, 128) for t in (2 * h, 1))
            x = jnp.concatenate([own, both], axis=0)
            x = x * (jnp.exp2(x[:, CHUNK : CHUNK + 1] * 0.125) * (1.0 / 32767.0))
            high = x.astype(jnp.bfloat16)
            low = (x - high.astype(jnp.float32)).astype(jnp.bfloat16)
            b_hi, b_lo = hi[h, 512 * half : 512 * half + 512, :], lo[h, 512 * half : 512 * half + 512, :]
            total = lax.dot_general(high, b_hi, dims, preferred_element_type=jnp.float32)
            total += lax.dot_general(low, b_hi, dims, preferred_element_type=jnp.float32)
            total += lax.dot_general(high, b_lo, dims, preferred_element_type=jnp.float32)
            totals[h] = total if half == 0 else totals[h] + total
    out_ref[:, 0:HALF] = (totals[0] + totals[1])[:CHUNK, :HALF]
    out_ref[:, HALF:LON] = (totals[0] - totals[1])[:CHUNK, :HALF]
    for c in sent:
        c.wait_send()
    for half in range(2):
        copy(send.at[half, most], held.at[half, most], fs.at[half], fr.at[half], along_z[1]).wait_send()


def body(pair_wave, legendre, coefs):
    vmem, hbm = pl.BlockSpec(memory_space=pltpu.VMEM), pl.BlockSpec(memory_space=pl.ANY)
    bf16, f32, dma = jnp.bfloat16, jnp.float32, pltpu.SemaphoreType.DMA
    return pl.pallas_call(
        kernel,
        out_shape=jax.ShapeDtypeStruct((CHUNK, LON), f32),
        in_specs=[pl.BlockSpec(memory_space=pltpu.SMEM), hbm, hbm],
        out_specs=vmem,
        scratch_shapes=[
            pltpu.VMEM((LAT_DEV, 45, 768), bf16),
            pltpu.VMEM((12, 45, 168), bf16),
            pltpu.VMEM((6, 480, 128), f32),
            pltpu.VMEM((6, 512, 128), f32),
            pltpu.VMEM((2, 576, 128), f32),
            pltpu.VMEM((4, 192, 128), f32),
            pltpu.VMEM((16, 32, 768), bf16),
            pltpu.VMEM((16, 3, 4, 512), bf16),
            pltpu.VMEM((8, 384), jnp.int32),
            pltpu.VMEM((ROWS, 128), f32),
            pltpu.VMEM((2, ROWS, 768), bf16),
            pltpu.VMEM((2, ROWS, 768), bf16),
            pltpu.VMEM((8, 32, 768), bf16),
            pltpu.VMEM((8, 32, 768), bf16),
            pltpu.VMEM((8, 8, 3, 4, 512), bf16),
            pltpu.VMEM((8, 8, 3, 4, 512), bf16),
            pltpu.VMEM((12, 256, 128), f32),
            pltpu.VMEM((768, 128), f32),
            pltpu.VMEM((2, 64, 3, 4, 128), jnp.int16),
            pltpu.VMEM((2, 64, 3, 4, 128), jnp.int16),
            dma((2,)),
            dma((2, 8)), dma((2, 8)), dma((2, 8)), dma((2, 8)),
            dma((2, 2, 4, 4)), dma((2, 2, 4, 4)), dma((2,)), dma((2,)),
        ],
        compiler_params=pltpu.CompilerParams(
            collective_id=0, has_side_effects=True, vmem_limit_bytes=60 * 2**20
        ),
    )(pair_wave, jnp.transpose(legendre, (1, 0, 2)), jnp.transpose(coefs, (1, 0, 2)))


def solution(mesh):
    placed = (P(), P("ma", "lat", None), P("ma", "lat", None))
    return jax.shard_map(
        body, mesh=mesh, in_specs=placed, out_specs=P(("lat", "ma"), None), check_vma=False
    )
```
